32 devices in a mesh: dom: 32 (over z, y, x, core).
Axes of the slice: x: 2, y: 2, z: 4, core: 2. Of those that a mesh axis runs over, the one named last changes fastest.
Arguments:
- right_side: float32 [18, 32768], P(None, 'dom'), may hold values from -20 to 20
- element_matrix: bfloat16 [72, 72, 16384], P(None, None, 'dom'), may hold values from -8 to 8, as said below
- face_map: int32 [4, 16384], P(None, 'dom'), may hold values from 0 to 1535
- share_index: int32 [32, 4, 128], P('dom'), may hold values from 0 to 1023
- share_count: int32 [32, 4], P('dom'), may hold values from 0 to 128, as said below
- face_mass: float32 [32768], P('dom'), may hold values from 0.5 to 2
- absorbing: int32 [32768], P('dom'), may hold values 0 or 1
- impedance: float32 [32768], P('dom'), may hold values from 0.5 to 4
Outputs:
- solution: float32 [18, 32768], P(None, 'dom')
- residual: float32 [18, 32768], P(None, 'dom')
The draws below stay inside these ranges and needn't reach their ends.
Inputs may be any that keep to these rules, and one draw needn't show every extreme that they name: `element_matrix`: each element's 72 x 72 matrix is symmetric positive definite. share_count[d, k] is 0 where device d + o_k lies outside the axis; it equals 128 for some device and offset in every draw.
All inputs are finite; a program needn't handle non-finite values. No bound on the sum of `absorbing` on one device may be relied on, other than what follows from the above.
Results may differ from the reference program's by a relative error of at most 0.0003.
Values sent between devices are 32-bit elements; how exact they have to be, the bound alone decides.
A program may use at most 64 MiB of HBM per device.

```python
import math
import jax
import jax.numpy as jnp
from jax import lax

TRACE = 18
SIDES = 4
DOFS = 72
REACH = 2
OFFSETS = 4
E_DEV = 512
F_DEV = 1024
GH = 128
ITERS = 2
E_TOTAL = 16384
F_TOTAL = 32768
N_DOM = 32


def draw_right_side(key, part):
    devices = F_TOTAL // F_DEV
    first_key, second_key, third_key = jax.random.split(key, 3)
    base_draw = jnp.clip(jax.random.normal(first_key, (TRACE, F_TOTAL), jnp.float32), -4.0, 4.0)
    component = jnp.exp(jax.random.uniform(second_key, (TRACE,), jnp.float32, jnp.log(0.5), jnp.log(5.0)))
    face_scale = jnp.exp(jax.random.uniform(third_key, (F_TOTAL,), jnp.float32, jnp.log(0.3), jnp.log(3.0)))
    device_of = jnp.arange(F_TOTAL, dtype=jnp.int32) // F_DEV
    ramp_scale = jnp.power(3.0, 0.5 * device_of.astype(jnp.float32) / (devices - 1))
    values_out = base_draw * component[:, None] * face_scale[None, :] * ramp_scale[None, :] * 0.25
    return jnp.clip(values_out, -20.0, 20.0).astype(jnp.float32)


def draw_element_matrix(key, part):
    devices = E_TOTAL // E_DEV

    def one_device(part_index):
        device_key = jax.random.fold_in(key, part_index)
        first_key, second_key = jax.random.split(device_key)
        raw_draw = jnp.clip(jax.random.normal(first_key, (DOFS, DOFS, E_DEV), jnp.float32), -5.0, 5.0)
        symmetric = 0.5 * (raw_draw + raw_draw.transpose(1, 0, 2)) * 0.025
        identity = jnp.eye(DOFS, dtype=jnp.float32)[:, :, None]
        off_diag = symmetric * (1.0 - identity)
        rowsum = jnp.sum(jnp.abs(off_diag), axis=1)
        stiffness = jnp.exp(jax.random.uniform(second_key, (E_DEV,), jnp.float32, jnp.log(0.5), jnp.log(2.0)))
        matrix = (off_diag + identity * (rowsum + 0.3)[:, None, :]) * stiffness[None, None, :]
        return matrix.astype(jnp.bfloat16)
    stacked = lax.map(one_device, jnp.arange(devices, dtype=jnp.int32))
    return jnp.moveaxis(stacked, 0, 2).reshape(DOFS, DOFS, E_TOTAL)


def draw_share_count(key, part):
    devices = F_TOTAL // F_DEV
    first_key, second_key, third_key, fourth_key = jax.random.split(key, 4)
    full_draw = jax.random.randint(first_key, (devices, OFFSETS), 0, 4)
    small_draw = jax.random.randint(second_key, (devices, OFFSETS), 0, GH // 4 + 1)
    counts = jnp.where(full_draw == 0, GH, small_draw)
    row_index = lax.broadcasted_iota(jnp.int32, (devices, OFFSETS), 0)
    blocks = lax.broadcasted_iota(jnp.int32, (devices, OFFSETS), 1)
    shift_by = jnp.where(blocks < REACH, blocks - REACH, blocks - REACH + 1)
    inside = (row_index + shift_by >= 0) & (row_index + shift_by < devices)
    pick_row = jax.random.randint(third_key, (), REACH, devices - REACH)
    pick_block = jax.random.randint(fourth_key, (), 0, OFFSETS)
    counts = jnp.where((row_index == pick_row) & (blocks == pick_block), GH, counts)
    return jnp.where(inside, counts, 0).astype(jnp.int32)


def touch_ends(entries, rng, smallest, top_value):
    shape = entries.shape
    index_at = [jax.random.randint(jax.random.fold_in(rng, axis), (), 0, shape[axis]) for axis in range(len(shape))]
    entries = entries.at[tuple(index_at)].set(smallest)
    longest = shape.index(max(shape))
    index_at[longest] = (index_at[longest] + 1) % shape[longest]
    return entries.at[tuple(index_at)].set(top_value)


def level_of(rng, shape, cuts, low, top_value):
    factor_of, own = 1.0, jax.random.fold_in(rng, 6)
    for axis_at, shards_of in cuts:
        heights = jnp.exp(jax.random.uniform(jax.random.fold_in(own, axis_at), (shards_of,), jnp.float32, low / len(cuts), top_value / len(cuts)))
        factor_of = factor_of * jnp.repeat(heights, shape[axis_at] // shards_of).reshape([-1 if axis == axis_at else 1 for axis in range(len(shape))])
    return factor_of


def setup_inputs(seed: int = 0) -> dict:
    streams_of = jax.random.split(jax.random.key(seed), 9)
    right_side = draw_right_side(jax.random.fold_in(streams_of[8], 71), 0)
    element_matrix = draw_element_matrix(jax.random.fold_in(streams_of[8], 71), 0)
    face_map = touch_ends(jax.random.randint(streams_of[2], (SIDES, E_TOTAL), 0, F_DEV + OFFSETS * GH), jax.random.fold_in(streams_of[2], 1), 0, (F_DEV + OFFSETS * GH) - 1).astype(jnp.int32)
    share_index = touch_ends(jax.random.randint(streams_of[3], (N_DOM, OFFSETS, GH), 0, F_DEV), jax.random.fold_in(streams_of[3], 1), 0, F_DEV - 1).astype(jnp.int32)
    share_count = draw_share_count(jax.random.fold_in(streams_of[8], 71), 0)
    face_mass = jnp.clip(jnp.exp(math.log(2.0) - 1.3862944 * jax.random.uniform(streams_of[5], (F_TOTAL,), jnp.float32) ** level_of(streams_of[5], (F_TOTAL,), ((0, 32),), -0.2, 0.2)), 0.5, 2.0)
    absorbing = touch_ends((jax.random.randint(streams_of[6], (F_TOTAL,), 0, 4) < 1).astype(jnp.int32), jax.random.fold_in(streams_of[6], 1), 0, 1)
    impedance = jnp.clip(jnp.exp(math.log(4.0) - 2.0794415 * jax.random.uniform(streams_of[7], (F_TOTAL,), jnp.float32) ** level_of(streams_of[7], (F_TOTAL,), ((0, 32),), -0.2, 0.2)), 0.5, 4.0)
    return {"right_side": right_side, "element_matrix": element_matrix, "face_map": face_map, "share_index": share_index, "share_count": share_count, "face_mass": face_mass, "absorbing": absorbing, "impedance": impedance}


def offset_of(block_index):
    return block_index - REACH if block_index < REACH else block_index - REACH + 1


def slot_map(face_map, share_index, share_count):
    element_count = face_map.shape[1]
    owner = jnp.arange(element_count, dtype=jnp.int32) // E_DEV
    owner = jnp.broadcast_to(owner[None, :], face_map.shape)
    local_face = face_map < F_DEV
    ghost_slot = jnp.maximum(face_map - F_DEV, 0)
    block_index = ghost_slot // GH
    within = ghost_slot % GH
    offsets = jnp.array([offset_of(b) for b in range(OFFSETS)], dtype=jnp.int32)
    sender = owner - offsets[block_index]
    sender_ok = (sender >= 0) & (sender < N_DOM)
    sender_safe = jnp.clip(sender, 0, N_DOM - 1).astype(jnp.int32)
    remote = share_index[sender_safe, block_index, within]
    live_count = share_count[sender_safe, block_index]
    alive_slot = sender_ok & (within < live_count)
    target = jnp.where(local_face, owner * F_DEV + face_map, sender_safe * F_DEV + remote).astype(jnp.int32)
    weight = jnp.where(local_face | alive_slot, 1.0, 0.0).astype(jnp.float32)
    return target, weight


def operate(field_now, element_matrix, target, weight, diagonal):
    picked = field_now[:, target] * weight[None, :, :]
    picked = picked.transpose(1, 0, 2).reshape(DOFS, E_TOTAL)

    def one_part(part_index):
        first_element = part_index * E_DEV
        matrices = lax.dynamic_slice_in_dim(element_matrix, first_element, E_DEV, 2).astype(jnp.float32)
        traces_in = lax.dynamic_slice_in_dim(picked, first_element, E_DEV, 1)
        return jnp.sum(matrices * traces_in[None, :, :], axis=1)

    products = lax.map(one_part, jnp.arange(N_DOM, dtype=jnp.int32))
    product = products.transpose(1, 0, 2).reshape(DOFS, E_TOTAL)
    spread = product.reshape(SIDES, TRACE, E_TOTAL) * weight[:, None, :]
    spread = spread.transpose(1, 0, 2)
    result = jnp.zeros_like(field_now).at[:, target].add(spread)
    return result + diagonal[None, :] * field_now


def reference(right_side, element_matrix, face_map, share_index, share_count, face_mass, absorbing, impedance):
    diagonal = face_mass + absorbing.astype(jnp.float32) * impedance
    target, weight = slot_map(face_map, share_index, share_count)
    solution = jnp.zeros_like(right_side)
    residual = right_side
    direction = right_side
    norm_now = jnp.sum(residual * residual)
    for rounds in range(ITERS):
        image_vec = operate(direction, element_matrix, target, weight, diagonal)
        step_size = norm_now / jnp.sum(direction * image_vec)
        solution = solution + step_size * direction
        residual = residual - step_size * image_vec
        norm_next = jnp.sum(residual * residual)
        direction = residual + (norm_next / norm_now) * direction
        norm_now = norm_next
    return solution, residual
```

```python
import functools
import jax
import jax.numpy as jnp
from jax import lax
from jax.experimental import pallas as pl
from jax.experimental.pallas import tpu as pltpu
from jax.sharding import PartitionSpec as P

LANES = 128
WIDE = 256
MESH = pl.DeviceIdType.MESH
F32 = jnp.float32
BF16 = jnp.bfloat16


def offset_list(block_count):
    half_count = block_count // 2
    return [
        block_index - half_count if block_index < half_count else block_index - half_count + 1
        for block_index in range(block_count)
    ]


def split3(x):
    high = x.astype(BF16)
    rest = x - high.astype(F32)
    middle = rest.astype(BF16)
    low = (rest - middle.astype(F32)).astype(BF16)
    return jnp.concatenate([high, middle, low], axis=0)


def sum3(x):
    rows = x.shape[0] // 3
    return x[:rows] + (x[rows : 2 * rows] + x[2 * rows :])


def dot(a, b):
    return lax.dot_general(a, b, (((1,), (0,)), ((), ())), preferred_element_type=F32)


def dot_nt(a, b):
    return lax.dot_general(a, b, (((1,), (1,)), ((), ())), preferred_element_type=F32)


def kernel(
    cfg,
    rs_ref, em_ref, fm_ref, si_ref, sc_ref, mass_ref, absorb_ref, imp_ref,
    sol_ref, res_ref,
    em_buf, pick_map, send_map, out_buf, ghost_buf, part_buf, ret_buf,
    picked, prod, spread_own, spread_ghost, b_buf, q_buf, sum1, sum2,
    em_sem, fetch_send, fetch_recv, ret_send, ret_recv,
    s1_send, s1_recv, s2_send, s2_recv,
):
    n, g1, g2, trace, sides, elements, own, blocks, width = cfg
    offsets = offset_list(blocks)
    pad = -(-trace // 8) * 8
    own_hi = own // WIDE
    ghost_hi = blocks * width // WIDE
    chunks = sides * elements // WIDE
    per_side = elements // WIDE
    rows_own, rows_ghost = own_hi * pad, ghost_hi * pad
    me = lax.axis_index("dom")
    block_of, in_block = me // g1, lax.rem(me, g1)

    em_copies = [
        pltpu.make_async_copy(
            em_ref.at[pl.ds(s * trace, trace)], em_buf.at[pl.ds(s * trace, trace)], em_sem.at[s]
        )
        for s in range(sides)
    ]
    for copy in em_copies:
        copy.start()

    barrier = pltpu.get_barrier_semaphore()
    waits = jnp.int32((g1 - 1) + (g2 - 1))
    for o in offsets:
        there = me + o
        inside = (there >= 0) & (there < n)
        waits = waits + inside.astype(jnp.int32)

        @pl.when(inside)
        def _():
            pl.semaphore_signal(barrier, inc=1, device_id=(there,), device_id_type=MESH)

    def peer1(d):
        return block_of * g1 + lax.rem(in_block + d, g1)

    def peer2(d):
        return lax.rem(block_of + d, g2) * g1 + in_block

    for d in range(1, g1):
        pl.semaphore_signal(barrier, inc=1, device_id=(peer1(d),), device_id_type=MESH)
    for d in range(1, g2):
        pl.semaphore_signal(barrier, inc=1, device_id=(peer2(d),), device_id_type=MESH)

    lo_iota = lax.broadcasted_iota(jnp.int32, (WIDE, WIDE), 0)
    slot_iota = lax.broadcasted_iota(jnp.int32, (1, width), 1)
    per_wide = WIDE // width
    send_hi = []
    for h in range(ghost_hi):
        cols = []
        for k in range(h * per_wide, (h + 1) * per_wide):
            alive = slot_iota < sc_ref[0:1, k : k + 1]
            cols.append(jnp.where(alive, si_ref[0, k : k + 1, :], -1))
        index = jnp.concatenate(cols, axis=1)
        low = jnp.where(index < 0, -1, index & (WIDE - 1))
        send_map[:, h * WIDE : (h + 1) * WIDE] = (lo_iota == low).astype(F32).astype(BF16)
        send_hi.append(index >> 8)

    def pick_hi(index, stacked, count):
        value = jnp.zeros((pad, WIDE), F32)
        for h in range(count):
            value = jnp.where(index == h, stacked[h * pad : (h + 1) * pad], value)
        return value

    def send_of(split, rnd):
        for h in range(ghost_hi):
            got = sum3(dot(split, send_map[:, h * WIDE : (h + 1) * WIDE]))
            out_buf[rnd, h * pad : (h + 1) * pad, :] = pick_hi(send_hi[h], got, own_hi)

    def piece(ref, rnd, k):
        h, lane = k // per_wide, (k % per_wide) * width
        return ref.at[rnd, pl.ds(h * pad, pad), pl.ds(lane, width)]

    def halo(src, dst, send_sem, recv_sem, rnd, k, step):
        there = me + step
        copy = pltpu.make_async_remote_copy(
            src_ref=piece(src, rnd, k), dst_ref=piece(dst, rnd, k),
            send_sem=send_sem.at[rnd, k], recv_sem=recv_sem.at[rnd, k],
            device_id=(there,), device_id_type=MESH,
        )
        came = me - step
        return copy, (there >= 0) & (there < n), (came >= 0) & (came < n)

    def fetch(rnd, k):
        return halo(out_buf, ghost_buf, fetch_send, fetch_recv, rnd, k, offsets[k])

    def giveback(rnd, k):
        return halo(part_buf, ret_buf, ret_send, ret_recv, rnd, k, -offsets[k])

    def start_all(make, rnd):
        for k in range(blocks):
            copy, to, _ = make(rnd, k)
            pl.when(to)(copy.start)

    def wait_recv_all(make, rnd):
        for k in range(blocks):
            copy, _, came = make(rnd, k)
            pl.when(came)(copy.wait_recv)

    def wait_send_all(make, rnd):
        for k in range(blocks):
            copy, to, _ = make(rnd, k)
            pl.when(to)(copy.wait_send)

    b_buf[...] = jnp.zeros_like(b_buf)
    for h in range(own_hi):
        b_buf[h * pad : h * pad + trace, :] = rs_ref[:, h * WIDE : (h + 1) * WIDE]
    b_split = split3(b_buf[...])
    send_of(b_split, 0)
    for k in range(blocks):
        for rnd in range(2):
            for ref, step in ((ghost_buf, offsets[k]), (ret_buf, -offsets[k])):
                came = me - step

                @pl.when((came < 0) | (came >= n))
                def _():
                    h, lane = k // per_wide, (k % per_wide) * width
                    ref[rnd, h * pad : (h + 1) * pad, lane : lane + width] = jnp.zeros(
                        (pad, width), F32
                    )

    pl.semaphore_wait(barrier, waits)
    start_all(fetch, 0)

    hi_of = []
    for c in range(chunks):
        s, lane = c // per_side, (c % per_side) * WIDE
        index = fm_ref[s : s + 1, lane : lane + WIDE]
        low = index & (WIDE - 1)
        pick_map[:, c * WIDE : (c + 1) * WIDE] = (lo_iota == low).astype(F32).astype(BF16)
        hi_of.append(index >> 8)
    prod[...] = jnp.zeros_like(prod)
    row_live = lax.broadcasted_iota(jnp.int32, (pad, WIDE), 0) < trace
    diag_row = mass_ref[...] + absorb_ref[...].astype(F32) * imp_ref[...]

    def diagonal_times(x):
        return jnp.concatenate(
            [
                x[h * pad : (h + 1) * pad] * diag_row[:, h * WIDE : (h + 1) * WIDE]
                for h in range(own_hi)
            ],
            axis=0,
        )

    def operate(x, split, rnd, before_wait, after_fetch, before_ret):
        for c in range(chunks):
            s, lane = c // per_side, (c % per_side) * WIDE
            got = sum3(dot(split, pick_map[:, c * WIDE : (c + 1) * WIDE]))
            picked[s, :, lane : lane + WIDE] = pick_hi(hi_of[c], got, own_hi)
        before_wait()
        wait_recv_all(fetch, rnd)
        ghost_split = split3(ghost_buf[rnd])
        for c in range(chunks):
            s, lane = c // per_side, (c % per_side) * WIDE
            got = sum3(dot(ghost_split, pick_map[:, c * WIDE : (c + 1) * WIDE]))
            picked[s, :, lane : lane + WIDE] += pick_hi(hi_of[c] - own_hi, got, ghost_hi)
        after_fetch()
        if rnd == 0:
            for copy in em_copies:
                copy.wait()
        for t in range(elements // LANES):
            lanes = slice(t * LANES, (t + 1) * LANES)

            def body(s, acc):
                for c in range(trace):
                    row = picked[s, c : c + 1, lanes]
                    acc = acc + em_buf[s * trace + c, :, lanes].astype(F32) * row
                return acc

            prod[0 : sides * trace, lanes] = lax.fori_loop(
                0, sides, body, jnp.zeros((sides * trace, LANES), F32)
            )

        def spread(c):
            s, lane = c // per_side, (c % per_side) * WIDE
            value = prod[s * trace : s * trace + pad, lane : lane + WIDE]
            return jnp.where(row_live, value, 0.0)

        for c in range(chunks):
            value = spread(c)
            stacked = jnp.concatenate(
                [jnp.where(hi_of[c] == own_hi + h, value, 0.0) for h in range(ghost_hi)], axis=0
            )
            spread_ghost[:, c * WIDE : (c + 1) * WIDE] = split3(stacked)
        part_buf[rnd] = sum3(dot_nt(spread_ghost[...], pick_map[...]))
        start_all(giveback, rnd)
        for c in range(chunks):
            value = spread(c)
            stacked = jnp.concatenate(
                [jnp.where(hi_of[c] == h, value, 0.0) for h in range(own_hi)], axis=0
            )
            spread_own[:, c * WIDE : (c + 1) * WIDE] = split3(stacked)
        result = sum3(dot_nt(spread_own[...], pick_map[...])) + diagonal_times(x)
        before_ret()
        wait_recv_all(giveback, rnd)
        for h in range(ghost_hi):
            value = ret_buf[rnd, h * pad : (h + 1) * pad, :]
            stacked = jnp.concatenate(
                [jnp.where(send_hi[h] == i, value, 0.0) for i in range(own_hi)], axis=0
            )
            result = result + sum3(
                dot_nt(split3(stacked), send_map[:, h * WIDE : (h + 1) * WIDE])
            )
        return result

    def stage1(rnd, d):
        slot = sum1.at[rnd, in_block]
        return pltpu.make_async_remote_copy(
            src_ref=slot, dst_ref=slot, send_sem=s1_send.at[rnd, d], recv_sem=s1_recv.at[rnd, d],
            device_id=(peer1(d),), device_id_type=MESH,
        )

    def stage2(rnd, d):
        slot = sum2.at[rnd, block_of]
        return pltpu.make_async_remote_copy(
            src_ref=slot, dst_ref=slot, send_sem=s2_send.at[rnd, d], recv_sem=s2_recv.at[rnd, d],
            device_id=(peer2(d),), device_id_type=MESH,
        )

    def lane_sums(x):
        total = jnp.sum(x, axis=0, keepdims=True)
        return total[:, :LANES] + total[:, LANES:]

    def begin_sum(rnd, x, y):
        sum1[rnd, in_block] = jnp.concatenate([lane_sums(x), lane_sums(y)], axis=0)
        for d in range(1, g1):
            stage1(rnd, d).start()

    def middle_sum(rnd):
        for d in range(1, g1):
            stage1(rnd, d).wait_recv()
        sum2[rnd, block_of] = jnp.sum(sum1[rnd], axis=0)
        for d in range(1, g2):
            stage2(rnd, d).start()

    def end_sum(rnd):
        for d in range(1, g2):
            stage2(rnd, d).wait_recv()
        total = jnp.sum(jnp.sum(sum2[rnd], axis=0), axis=1, keepdims=True)
        return total[0:1], total[1:2]

    nothing = lambda: None
    q = operate(b_buf[...], b_split, 0, nothing, nothing, nothing)
    q_buf[...] = q
    q_split = split3(q)
    send_of(q_split, 1)
    start_all(fetch, 1)
    b = b_buf[...]
    begin_sum(0, b * b, b * q)
    w = operate(q_buf[...], q_split, 1, nothing, lambda: middle_sum(0), nothing)
    rr, curve = end_sum(0)
    step0 = rr / curve
    b, q = b_buf[...], q_buf[...]
    r1 = b - step0 * q
    z1 = q - step0 * w
    begin_sum(1, r1 * r1, r1 * z1)
    middle_sum(1)
    new, curve = end_sum(1)
    beta = new / rr
    step1 = new / (curve - beta * new / step0)
    sol = step0 * b + step1 * (r1 + beta * b)
    res = r1 - step1 * (z1 + beta * q)
    for h in range(own_hi):
        sol_ref[:, h * WIDE : (h + 1) * WIDE] = sol[h * pad : h * pad + trace]
        res_ref[:, h * WIDE : (h + 1) * WIDE] = res[h * pad : h * pad + trace]
    for rnd in range(2):
        wait_send_all(fetch, rnd)
        wait_send_all(giveback, rnd)
        for d in range(1, g1):
            stage1(rnd, d).wait_send()
        for d in range(1, g2):
            stage2(rnd, d).wait_send()


def solution(mesh):
    n = mesh.shape["dom"]
    g1 = next(g for g in range(1, n + 1) if n % g == 0 and g * g >= n)
    g2 = n // g1

    def shards(rs, em, fm, si, sc, mass, absorb, imp):
        trace, own = rs.shape
        sides, elements = fm.shape
        blocks, width = si.shape[1:]
        pad = -(-trace // 8) * 8
        rows_own = own // WIDE * pad
        rows_ghost = blocks * width // WIDE * pad
        picks = sides * elements
        dofs = sides * trace
        cfg = (n, g1, g2, trace, sides, elements, own, blocks, width)
        dma = pltpu.SemaphoreType.DMA
        vmem = pl.BlockSpec(memory_space=pltpu.VMEM)
        return pl.pallas_call(
            functools.partial(kernel, cfg),
            out_shape=[jax.ShapeDtypeStruct(rs.shape, F32)] * 2,
            in_specs=[vmem, pl.BlockSpec(memory_space=pl.ANY)] + [vmem] * 6,
            out_specs=[vmem] * 2,
            scratch_shapes=[
                pltpu.VMEM((dofs, dofs, elements), BF16),
                pltpu.VMEM((WIDE, picks), BF16),
                pltpu.VMEM((WIDE, blocks * width), BF16),
                pltpu.VMEM((2, rows_ghost, WIDE), F32),
                pltpu.VMEM((2, rows_ghost, WIDE), F32),
                pltpu.VMEM((2, rows_ghost, WIDE), F32),
                pltpu.VMEM((2, rows_ghost, WIDE), F32),
                pltpu.VMEM((sides, pad, elements), F32),
                pltpu.VMEM((dofs + 8, elements), F32),
                pltpu.VMEM((3 * rows_own, picks), BF16),
                pltpu.VMEM((3 * rows_ghost, picks), BF16),
                pltpu.VMEM((rows_own, WIDE), F32),
                pltpu.VMEM((rows_own, WIDE), F32),
                pltpu.VMEM((2, g1, 2, LANES), F32),
                pltpu.VMEM((2, g2, 2, LANES), F32),
                dma((sides,)),
                dma((2, blocks)), dma((2, blocks)), dma((2, blocks)), dma((2, blocks)),
                dma((2, g1)), dma((2, g1)), dma((2, g2)), dma((2, g2)),
            ],
            compiler_params=pltpu.CompilerParams(
                collective_id=0, has_side_effects=True, vmem_limit_bytes=62 * 1024 * 1024
            ),
        )(rs, em, fm, si, sc, mass.reshape(1, own), absorb.reshape(1, own), imp.reshape(1, own))

    placed = (
        P(None, "dom"),
        P(None, None, "dom"),
        P(None, "dom"),
        P("dom", None, None),
        P("dom", None),
        P("dom"),
        P("dom"),
        P("dom"),
    )
    return jax.shard_map(
        shards,
        mesh=mesh,
        in_specs=placed,
        out_specs=(P(None, "dom"), P(None, "dom")),
        check_vma=False,
    )
```

```python
import functools
import jax
import jax.numpy as jnp
from jax import lax
from jax.experimental import pallas as pl
from jax.experimental.pallas import tpu as pltpu
from jax.sharding import PartitionSpec as P

LANES = 128
WIDE = 256
MESH = pl.DeviceIdType.MESH
F32 = jnp.float32
BF16 = jnp.bfloat16


def offset_list(block_count):
    half_count = block_count // 2
    return [
        block_index - half_count if block_index < half_count else block_index - half_count + 1
        for block_index in range(block_count)
    ]


def split3(x):
    high = x.astype(BF16)
    rest = x - high.astype(F32)
    middle = rest.astype(BF16)
    low = (rest - middle.astype(F32)).astype(BF16)
    return jnp.concatenate([high, middle, low], axis=0)


def sum3(x):
    rows = x.shape[0] // 3
    return x[:rows] + (x[rows : 2 * rows] + x[2 * rows :])


def dot(a, b):
    return lax.dot_general(a, b, (((1,), (0,)), ((), ())), preferred_element_type=F32)


def dot_nt(a, b):
    return lax.dot_general(a, b, (((1,), (1,)), ((), ())), preferred_element_type=F32)


def kernel(
    cfg,
    rs_in, em_ref, fm_in, si_in, sc_in, mass_in, absorb_in, imp_in,
    sol_ref, res_ref,
    rs_ref, fm_ref, si_ref, sc_ref, mass_ref, absorb_ref, imp_ref,
    em_buf, pick_map, send_map, out_buf, ghost_buf, part_buf, ret_buf,
    picked, prod, spread_own, spread_ghost, b_buf, q_buf, sum1, sum2, sum_all,
    in_sem, em_sem, fetch_send, fetch_recv, ret_send, ret_recv,
    s1_send, s1_recv, s2_send, s2_recv, all_send, all_recv,
):
    n, g1, g2, trace, sides, elements, own, blocks, width = cfg
    offsets = offset_list(blocks)
    pad = -(-trace // 8) * 8
    own_hi = own // WIDE
    ghost_hi = blocks * width // WIDE
    chunks = sides * elements // WIDE
    per_side = elements // WIDE
    rows_own, rows_ghost = own_hi * pad, ghost_hi * pad
    me = lax.axis_index("dom")
    block_of, in_block = me // g1, lax.rem(me, g1)

    barrier = pltpu.get_barrier_semaphore()
    waits = jnp.int32((g1 - 1) + (g2 - 1))
    for o in offsets:
        there = me + o
        inside = (there >= 0) & (there < n)
        waits = waits + inside.astype(jnp.int32)

        @pl.when(inside)
        def _():
            pl.semaphore_signal(barrier, inc=1, device_id=(there,), device_id_type=MESH)

    def peer1(d):
        return block_of * g1 + lax.rem(in_block + d, g1)

    def peer2(d):
        return lax.rem(block_of + d, g2) * g1 + in_block

    for d in range(1, g1):
        pl.semaphore_signal(barrier, inc=1, device_id=(peer1(d),), device_id_type=MESH)
    for d in range(1, g2):
        pl.semaphore_signal(barrier, inc=1, device_id=(peer2(d),), device_id_type=MESH)

    in_copies = [
        pltpu.make_async_copy(source, target, in_sem.at[i])
        for i, (source, target) in enumerate(
            (
                (rs_in, rs_ref), (si_in, si_ref), (sc_in, sc_ref), (fm_in, fm_ref),
                (mass_in, mass_ref), (absorb_in, absorb_ref), (imp_in, imp_ref),
            )
        )
    ]
    for copy in in_copies:
        copy.start()
    em_copies = [
        pltpu.make_async_copy(
            em_ref.at[pl.ds(s * trace, trace)], em_buf.at[pl.ds(s * trace, trace)], em_sem.at[s]
        )
        for s in range(sides)
    ]
    for copy in em_copies:
        copy.start()

    for copy in in_copies[:3]:
        copy.wait()
    lo_iota = lax.broadcasted_iota(jnp.int32, (WIDE, WIDE), 0)
    slot_iota = lax.broadcasted_iota(jnp.int32, (1, width), 1)
    per_wide = WIDE // width
    send_hi = []
    for h in range(ghost_hi):
        cols = []
        for k in range(h * per_wide, (h + 1) * per_wide):
            alive = slot_iota < sc_ref[0:1, k : k + 1]
            cols.append(jnp.where(alive, si_ref[0, k : k + 1, :], -1))
        index = jnp.concatenate(cols, axis=1)
        low = jnp.where(index < 0, -1, index & (WIDE - 1))
        send_map[:, h * WIDE : (h + 1) * WIDE] = (lo_iota == low).astype(F32).astype(BF16)
        send_hi.append(index >> 8)

    def pick_hi(index, stacked, count):
        value = jnp.zeros((pad, WIDE), F32)
        for h in range(count):
            value = jnp.where(index == h, stacked[h * pad : (h + 1) * pad], value)
        return value

    def send_of(split, rnd):
        for h in range(ghost_hi):
            got = sum3(dot(split, send_map[:, h * WIDE : (h + 1) * WIDE]))
            out_buf[rnd, h * pad : (h + 1) * pad, :] = pick_hi(send_hi[h], got, own_hi)

    def piece(ref, rnd, k):
        h, lane = k // per_wide, (k % per_wide) * width
        return ref.at[rnd, pl.ds(h * pad, pad), pl.ds(lane, width)]

    def halo(src, dst, send_sem, recv_sem, rnd, k, step):
        there = me + step
        copy = pltpu.make_async_remote_copy(
            src_ref=piece(src, rnd, k), dst_ref=piece(dst, rnd, k),
            send_sem=send_sem.at[rnd, k], recv_sem=recv_sem.at[rnd, k],
            device_id=(there,), device_id_type=MESH,
        )
        came = me - step
        return copy, (there >= 0) & (there < n), (came >= 0) & (came < n)

    def fetch(rnd, k):
        return halo(out_buf, ghost_buf, fetch_send, fetch_recv, rnd, k, offsets[k])

    def giveback(rnd, k):
        return halo(part_buf, ret_buf, ret_send, ret_recv, rnd, k, -offsets[k])

    def start_all(make, rnd):
        for k in range(blocks):
            copy, to, _ = make(rnd, k)
            pl.when(to)(copy.start)

    def wait_recv_all(make, rnd):
        for k in range(blocks):
            copy, _, came = make(rnd, k)
            pl.when(came)(copy.wait_recv)

    def wait_send_all(make, rnd):
        for k in range(blocks):
            copy, to, _ = make(rnd, k)
            pl.when(to)(copy.wait_send)

    b_buf[...] = jnp.zeros_like(b_buf)
    for h in range(own_hi):
        b_buf[h * pad : h * pad + trace, :] = rs_ref[:, h * WIDE : (h + 1) * WIDE]
    b_split = split3(b_buf[...])
    send_of(b_split, 0)
    for k in range(blocks):
        for rnd in range(2):
            for ref, step in ((ghost_buf, offsets[k]), (ret_buf, -offsets[k])):
                came = me - step

                @pl.when((came < 0) | (came >= n))
                def _():
                    h, lane = k // per_wide, (k % per_wide) * width
                    ref[rnd, h * pad : (h + 1) * pad, lane : lane + width] = jnp.zeros(
                        (pad, width), F32
                    )

    pl.semaphore_wait(barrier, waits)
    start_all(fetch, 0)

    for copy in in_copies[3:]:
        copy.wait()
    hi_of = []
    for c in range(chunks):
        s, lane = c // per_side, (c % per_side) * WIDE
        index = fm_ref[s : s + 1, lane : lane + WIDE]
        low = index & (WIDE - 1)
        pick_map[:, c * WIDE : (c + 1) * WIDE] = (lo_iota == low).astype(F32).astype(BF16)
        hi_of.append(index >> 8)
    prod[...] = jnp.zeros_like(prod)
    row_live = lax.broadcasted_iota(jnp.int32, (pad, WIDE), 0) < trace
    diag_row = mass_ref[...] + absorb_ref[...].astype(F32) * imp_ref[...]

    def diagonal_times(x):
        return jnp.concatenate(
            [
                x[h * pad : (h + 1) * pad] * diag_row[:, h * WIDE : (h + 1) * WIDE]
                for h in range(own_hi)
            ],
            axis=0,
        )

    def operate(x, split, rnd, after_product):
        for c in range(chunks):
            s, lane = c // per_side, (c % per_side) * WIDE
            got = sum3(dot(split, pick_map[:, c * WIDE : (c + 1) * WIDE]))
            picked[s, :, lane : lane + WIDE] = pick_hi(hi_of[c], got, own_hi)
        wait_recv_all(fetch, rnd)
        ghost_split = split3(ghost_buf[rnd])
        for c in range(chunks):
            s, lane = c // per_side, (c % per_side) * WIDE
            got = sum3(dot(ghost_split, pick_map[:, c * WIDE : (c + 1) * WIDE]))
            picked[s, :, lane : lane + WIDE] += pick_hi(hi_of[c] - own_hi, got, ghost_hi)
        if rnd == 0:
            for copy in em_copies:
                copy.wait()
        for t in range(elements // LANES):
            lanes = slice(t * LANES, (t + 1) * LANES)

            def body(s, acc):
                for c in range(trace):
                    row = picked[s, c : c + 1, lanes]
                    acc = acc + em_buf[s * trace + c, :, lanes].astype(F32) * row
                return acc

            prod[0 : sides * trace, lanes] = lax.fori_loop(
                0, sides, body, jnp.zeros((sides * trace, LANES), F32)
            )

        def spread(c):
            s, lane = c // per_side, (c % per_side) * WIDE
            value = prod[s * trace : s * trace + pad, lane : lane + WIDE]
            return jnp.where(row_live, value, 0.0)

        after_product()
        for c in range(chunks):
            value = spread(c)
            stacked = jnp.concatenate(
                [jnp.where(hi_of[c] == own_hi + h, value, 0.0) for h in range(ghost_hi)], axis=0
            )
            spread_ghost[:, c * WIDE : (c + 1) * WIDE] = split3(stacked)
        part_buf[rnd] = sum3(dot_nt(spread_ghost[...], pick_map[...]))
        start_all(giveback, rnd)
        for c in range(chunks):
            value = spread(c)
            stacked = jnp.concatenate(
                [jnp.where(hi_of[c] == h, value, 0.0) for h in range(own_hi)], axis=0
            )
            spread_own[:, c * WIDE : (c + 1) * WIDE] = split3(stacked)
        result = sum3(dot_nt(spread_own[...], pick_map[...])) + diagonal_times(x)
        wait_recv_all(giveback, rnd)
        for h in range(ghost_hi):
            value = ret_buf[rnd, h * pad : (h + 1) * pad, :]
            stacked = jnp.concatenate(
                [jnp.where(send_hi[h] == i, value, 0.0) for i in range(own_hi)], axis=0
            )
            result = result + sum3(
                dot_nt(split3(stacked), send_map[:, h * WIDE : (h + 1) * WIDE])
            )
        return result

    def stage1(d):
        slot = sum1.at[in_block]
        return pltpu.make_async_remote_copy(
            src_ref=slot, dst_ref=slot, send_sem=s1_send.at[d], recv_sem=s1_recv.at[d],
            device_id=(peer1(d),), device_id_type=MESH,
        )

    def stage2(d):
        slot = sum2.at[block_of]
        return pltpu.make_async_remote_copy(
            src_ref=slot, dst_ref=slot, send_sem=s2_send.at[d], recv_sem=s2_recv.at[d],
            device_id=(peer2(d),), device_id_type=MESH,
        )

    def lane_sums(x):
        total = jnp.sum(x, axis=0, keepdims=True)
        return total[:, :LANES] + total[:, LANES:]

    def pair_of(x, y):
        return jnp.concatenate([lane_sums(x), lane_sums(y)], axis=0)

    def begin_sum(x, y):
        sum1[in_block] = pair_of(x, y)
        for d in range(1, g1):
            stage1(d).start()

    def middle_sum():
        for d in range(1, g1):
            stage1(d).wait_recv()
        sum2[block_of] = jnp.sum(sum1[...], axis=0)
        for d in range(1, g2):
            stage2(d).start()

    def totals(parts):
        total = jnp.sum(jnp.sum(parts, axis=0), axis=1, keepdims=True)
        return total[0:1], total[1:2]

    def end_sum():
        for d in range(1, g2):
            stage2(d).wait_recv()
        return totals(sum2[...])

    def straight(d):
        return pltpu.make_async_remote_copy(
            src_ref=sum_all.at[0], dst_ref=sum_all.at[d],
            send_sem=all_send.at[d], recv_sem=all_recv.at[d],
            device_id=(lax.rem(me + d, n),), device_id_type=MESH,
        )

    def sum_straight(x, y):
        sum_all[0] = pair_of(x, y)
        for d in range(1, n):
            straight(d).start()
        for d in range(1, n):
            straight(d).wait_recv()
        return totals(sum_all[...])

    q = operate(b_buf[...], b_split, 0, lambda: None)
    q_buf[...] = q
    q_split = split3(q)
    send_of(q_split, 1)
    start_all(fetch, 1)
    b = b_buf[...]
    begin_sum(b * b, b * q)
    w = operate(q_buf[...], q_split, 1, middle_sum)
    rr, curve = end_sum()
    step0 = rr / curve
    b, q = b_buf[...], q_buf[...]
    r1 = b - step0 * q
    z1 = q - step0 * w
    new, curve = sum_straight(r1 * r1, r1 * z1)
    beta = new / rr
    step1 = new / (curve - beta * new / step0)
    sol = step0 * b + step1 * (r1 + beta * b)
    res = r1 - step1 * (z1 + beta * q)
    for h in range(own_hi):
        sol_ref[:, h * WIDE : (h + 1) * WIDE] = sol[h * pad : h * pad + trace]
        res_ref[:, h * WIDE : (h + 1) * WIDE] = res[h * pad : h * pad + trace]
    for rnd in range(2):
        wait_send_all(fetch, rnd)
        wait_send_all(giveback, rnd)
    for d in range(1, g1):
        stage1(d).wait_send()
    for d in range(1, g2):
        stage2(d).wait_send()
    for d in range(1, n):
        straight(d).wait_send()


def put_out(sol_ref, res_ref, sol_out, res_out, sems):
    copies = [
        pltpu.make_async_copy(sol_ref, sol_out, sems.at[0]),
        pltpu.make_async_copy(res_ref, res_out, sems.at[1]),
    ]
    for copy in copies:
        copy.start()
    for copy in copies:
        copy.wait()


def solution(mesh):
    n = mesh.shape["dom"]
    g1 = next(g for g in range(1, n + 1) if n % g == 0 and g * g >= n)
    g2 = n // g1

    def shards(rs, em, fm, si, sc, mass, absorb, imp):
        trace, own = rs.shape
        sides, elements = fm.shape
        blocks, width = si.shape[1:]
        pad = -(-trace // 8) * 8
        rows_own = own // WIDE * pad
        rows_ghost = blocks * width // WIDE * pad
        picks = sides * elements
        dofs = sides * trace
        cfg = (n, g1, g2, trace, sides, elements, own, blocks, width)
        dma = pltpu.SemaphoreType.DMA
        vmem = pl.BlockSpec(memory_space=pltpu.VMEM)
        sol, res = pl.pallas_call(
            functools.partial(kernel, cfg),
            out_shape=[pltpu.VMEM(rs.shape, F32)] * 2,
            in_specs=[pl.BlockSpec(memory_space=pltpu.HBM)] * 8,
            out_specs=[vmem] * 2,
            scratch_shapes=[
                pltpu.VMEM(rs.shape, F32),
                pltpu.VMEM(fm.shape, jnp.int32),
                pltpu.VMEM(si.shape, jnp.int32),
                pltpu.VMEM(sc.shape, jnp.int32),
                pltpu.VMEM((1, own), F32),
                pltpu.VMEM((1, own), jnp.int32),
                pltpu.VMEM((1, own), F32),
                pltpu.VMEM((dofs, dofs, elements), BF16),
                pltpu.VMEM((WIDE, picks), BF16),
                pltpu.VMEM((WIDE, blocks * width), BF16),
                pltpu.VMEM((2, rows_ghost, WIDE), F32),
                pltpu.VMEM((2, rows_ghost, WIDE), F32),
                pltpu.VMEM((2, rows_ghost, WIDE), F32),
                pltpu.VMEM((2, rows_ghost, WIDE), F32),
                pltpu.VMEM((sides, pad, elements), F32),
                pltpu.VMEM((dofs + 8, elements), F32),
                pltpu.VMEM((3 * rows_own, picks), BF16),
                pltpu.VMEM((3 * rows_ghost, picks), BF16),
                pltpu.VMEM((rows_own, WIDE), F32),
                pltpu.VMEM((rows_own, WIDE), F32),
                pltpu.VMEM((g1, 2, LANES), F32),
                pltpu.VMEM((g2, 2, LANES), F32),
                pltpu.VMEM((n, 2, LANES), F32),
                dma((7,)), dma((sides,)),
                dma((2, blocks)), dma((2, blocks)), dma((2, blocks)), dma((2, blocks)),
                dma((g1,)), dma((g1,)), dma((g2,)), dma((g2,)), dma((n,)), dma((n,)),
            ],
            compiler_params=pltpu.CompilerParams(
                collective_id=0, has_side_effects=True, vmem_limit_bytes=62 * 1024 * 1024
            ),
        )(rs, em, fm, si, sc, mass.reshape(1, own), absorb.reshape(1, own), imp.reshape(1, own))
        return pl.pallas_call(
            put_out,
            out_shape=[jax.ShapeDtypeStruct(rs.shape, F32)] * 2,
            in_specs=[vmem] * 2,
            out_specs=[pl.BlockSpec(memory_space=pltpu.HBM)] * 2,
            scratch_shapes=[dma((2,))],
            compiler_params=pltpu.CompilerParams(vmem_limit_bytes=8 * 1024 * 1024),
        )(sol, res)

    placed = (
        P(None, "dom"),
        P(None, None, "dom"),
        P(None, "dom"),
        P("dom", None, None),
        P("dom", None),
        P("dom"),
        P("dom"),
        P("dom"),
    )
    return jax.shard_map(
        shards,
        mesh=mesh,
        in_specs=placed,
        out_specs=(P(None, "dom"), P(None, "dom")),
        check_vma=False,
    )
```

```python
import functools
import jax
import jax.numpy as jnp
from jax import lax
from jax.experimental import pallas as pl
from jax.experimental.pallas import tpu as pltpu
from jax.sharding import PartitionSpec as P

LANES = 128
WIDE = 256
MESH = pl.DeviceIdType.MESH
F32 = jnp.float32
BF16 = jnp.bfloat16


def offset_list(block_count):
    half_count = block_count // 2
    return [
        block_index - half_count if block_index < half_count else block_index - half_count + 1
        for block_index in range(block_count)
    ]


def split3(x):
    high = x.astype(BF16)
    rest = x - high.astype(F32)
    middle = rest.astype(BF16)
    low = (rest - middle.astype(F32)).astype(BF16)
    return jnp.concatenate([high, middle, low], axis=0)


def sum3(x):
    rows = x.shape[0] // 3
    return x[:rows] + (x[rows : 2 * rows] + x[2 * rows :])


def dot(a, b):
    return lax.dot_general(a, b, (((1,), (0,)), ((), ())), preferred_element_type=F32)


def dot_nt(a, b):
    return lax.dot_general(a, b, (((1,), (1,)), ((), ())), preferred_element_type=F32)


def kernel(
    cfg,
    rs_in, em_ref, fm_in, si_in, sc_in, mass_in, absorb_in, imp_in,
    sol_ref, res_ref,
    rs_ref, fm_ref, si_ref, sc_ref, mass_ref, absorb_ref, imp_ref,
    em_buf, pick_map, send_map, out_buf, ghost_buf, part_buf, ret_buf,
    picked, prod, spread_own, spread_ghost, b_buf, q_buf, sum1, sum2, sum_all,
    in_sem, em_sem, fetch_send, fetch_recv, ret_send, ret_recv,
    s1_send, s1_recv, s2_send, s2_recv, all_send, all_recv,
):
    n, g1, g2, trace, sides, elements, own, blocks, width = cfg
    offsets = offset_list(blocks)
    pad = -(-trace // 8) * 8
    own_hi = own // WIDE
    ghost_hi = blocks * width // WIDE
    chunks = sides * elements // WIDE
    per_side = elements // WIDE
    rows_own, rows_ghost = own_hi * pad, ghost_hi * pad
    me = lax.axis_index("dom")
    block_of, in_block = me // g1, lax.rem(me, g1)

    barrier = pltpu.get_barrier_semaphore()
    waits = jnp.int32((g1 - 1) + (g2 - 1))
    for o in offsets:
        there = me + o
        inside = (there >= 0) & (there < n)
        waits = waits + inside.astype(jnp.int32)

        @pl.when(inside)
        def _():
            pl.semaphore_signal(barrier, inc=1, device_id=(there,), device_id_type=MESH)

    def peer1(d):
        return block_of * g1 + lax.rem(in_block + d, g1)

    def peer2(d):
        return lax.rem(block_of + d, g2) * g1 + in_block

    for d in range(1, g1):
        pl.semaphore_signal(barrier, inc=1, device_id=(peer1(d),), device_id_type=MESH)
    for d in range(1, g2):
        pl.semaphore_signal(barrier, inc=1, device_id=(peer2(d),), device_id_type=MESH)

    in_copies = [
        pltpu.make_async_copy(source, target, in_sem.at[i])
        for i, (source, target) in enumerate(
            (
                (rs_in, rs_ref), (si_in, si_ref), (sc_in, sc_ref), (fm_in, fm_ref),
                (mass_in, mass_ref), (absorb_in, absorb_ref), (imp_in, imp_ref),
            )
        )
    ]
    for copy in in_copies:
        copy.start()
    em_copies = [
        pltpu.make_async_copy(
            em_ref.at[pl.ds(s * trace, trace)], em_buf.at[pl.ds(s * trace, trace)], em_sem.at[s]
        )
        for s in range(sides)
    ]
    for copy in em_copies:
        copy.start()

    for copy in in_copies[:3]:
        copy.wait()
    lo_iota = lax.broadcasted_iota(jnp.int32, (WIDE, WIDE), 0)
    slot_iota = lax.broadcasted_iota(jnp.int32, (1, width), 1)
    per_wide = WIDE // width
    send_hi = []
    for h in range(ghost_hi):
        cols = []
        for k in range(h * per_wide, (h + 1) * per_wide):
            alive = slot_iota < sc_ref[0:1, k : k + 1]
            cols.append(jnp.where(alive, si_ref[0, k : k + 1, :], -1))
        index = jnp.concatenate(cols, axis=1)
        low = jnp.where(index < 0, -1, index & (WIDE - 1))
        send_map[:, h * WIDE : (h + 1) * WIDE] = (lo_iota == low).astype(F32).astype(BF16)
        send_hi.append(index >> 8)

    def pick_hi(index, stacked, count):
        value = jnp.zeros((pad, WIDE), F32)
        for h in range(count):
            value = jnp.where(index == h, stacked[h * pad : (h + 1) * pad], value)
        return value

    def send_of(split, rnd):
        for h in range(ghost_hi):
            got = sum3(dot(split, send_map[:, h * WIDE : (h + 1) * WIDE]))
            out_buf[rnd, h * pad : (h + 1) * pad, :] = pick_hi(send_hi[h], got, own_hi)

    def piece(ref, rnd, k):
        h, lane = k // per_wide, (k % per_wide) * width
        return ref.at[rnd, pl.ds(h * pad, pad), pl.ds(lane, width)]

    def halo(src, dst, send_sem, recv_sem, rnd, k, step):
        there = me + step
        copy = pltpu.make_async_remote_copy(
            src_ref=piece(src, rnd, k), dst_ref=piece(dst, rnd, k),
            send_sem=send_sem.at[rnd, k], recv_sem=recv_sem.at[rnd, k],
            device_id=(there,), device_id_type=MESH,
        )
        came = me - step
        return copy, (there >= 0) & (there < n), (came >= 0) & (came < n)

    def fetch(rnd, k):
        return halo(out_buf, ghost_buf, fetch_send, fetch_recv, rnd, k, offsets[k])

    def giveback(rnd, k):
        return halo(part_buf, ret_buf, ret_send, ret_recv, rnd, k, -offsets[k])

    far_first = sorted(range(blocks), key=lambda k: -abs(offsets[k]))

    def start_all(make, rnd):
        for k in far_first:
            copy, to, _ = make(rnd, k)
            pl.when(to)(copy.start)

    def wait_recv_all(make, rnd):
        for k in range(blocks):
            copy, _, came = make(rnd, k)
            pl.when(came)(copy.wait_recv)

    def wait_send_all(make, rnd):
        for k in range(blocks):
            copy, to, _ = make(rnd, k)
            pl.when(to)(copy.wait_send)

    b_buf[...] = jnp.zeros_like(b_buf)
    for h in range(own_hi):
        b_buf[h * pad : h * pad + trace, :] = rs_ref[:, h * WIDE : (h + 1) * WIDE]
    b_split = split3(b_buf[...])
    send_of(b_split, 0)
    for k in range(blocks):
        for rnd in range(2):
            for ref, step in ((ghost_buf, offsets[k]), (ret_buf, -offsets[k])):
                came = me - step

                @pl.when((came < 0) | (came >= n))
                def _():
                    h, lane = k // per_wide, (k % per_wide) * width
                    ref[rnd, h * pad : (h + 1) * pad, lane : lane + width] = jnp.zeros(
                        (pad, width), F32
                    )

    pl.semaphore_wait(barrier, waits)
    start_all(fetch, 0)

    for copy in in_copies[3:]:
        copy.wait()
    hi_of = []
    for c in range(chunks):
        s, lane = c // per_side, (c % per_side) * WIDE
        index = fm_ref[s : s + 1, lane : lane + WIDE]
        low = index & (WIDE - 1)
        pick_map[:, c * WIDE : (c + 1) * WIDE] = (lo_iota == low).astype(F32).astype(BF16)
        hi_of.append(index >> 8)
    prod[...] = jnp.zeros_like(prod)
    row_live = lax.broadcasted_iota(jnp.int32, (pad, WIDE), 0) < trace
    diag_row = mass_ref[...] + absorb_ref[...].astype(F32) * imp_ref[...]

    def diagonal_times(x):
        return jnp.concatenate(
            [
                x[h * pad : (h + 1) * pad] * diag_row[:, h * WIDE : (h + 1) * WIDE]
                for h in range(own_hi)
            ],
            axis=0,
        )

    def operate(x, split, rnd, after_product):
        for c in range(chunks):
            s, lane = c // per_side, (c % per_side) * WIDE
            got = sum3(dot(split, pick_map[:, c * WIDE : (c + 1) * WIDE]))
            picked[s, :, lane : lane + WIDE] = pick_hi(hi_of[c], got, own_hi)
        wait_recv_all(fetch, rnd)
        ghost_split = split3(ghost_buf[rnd])
        for c in range(chunks):
            s, lane = c // per_side, (c % per_side) * WIDE
            got = sum3(dot(ghost_split, pick_map[:, c * WIDE : (c + 1) * WIDE]))
            picked[s, :, lane : lane + WIDE] += pick_hi(hi_of[c] - own_hi, got, ghost_hi)
        if rnd == 0:
            for copy in em_copies:
                copy.wait()
        for t in range(elements // LANES):
            lanes = slice(t * LANES, (t + 1) * LANES)

            def body(s, acc):
                for c in range(trace):
                    row = picked[s, c : c + 1, lanes]
                    acc = acc + em_buf[s * trace + c, :, lanes].astype(F32) * row
                return acc

            prod[0 : sides * trace, lanes] = lax.fori_loop(
                0, sides, body, jnp.zeros((sides * trace, LANES), F32)
            )

        def spread(c):
            s, lane = c // per_side, (c % per_side) * WIDE
            value = prod[s * trace : s * trace + pad, lane : lane + WIDE]
            return jnp.where(row_live, value, 0.0)

        after_product()
        for c in range(chunks):
            value = spread(c)
            stacked = jnp.concatenate(
                [jnp.where(hi_of[c] == own_hi + h, value, 0.0) for h in range(ghost_hi)], axis=0
            )
            spread_ghost[:, c * WIDE : (c + 1) * WIDE] = split3(stacked)
        part_buf[rnd] = sum3(dot_nt(spread_ghost[...], pick_map[...]))
        start_all(giveback, rnd)
        for c in range(chunks):
            value = spread(c)
            stacked = jnp.concatenate(
                [jnp.where(hi_of[c] == h, value, 0.0) for h in range(own_hi)], axis=0
            )
            spread_own[:, c * WIDE : (c + 1) * WIDE] = split3(stacked)
        result = sum3(dot_nt(spread_own[...], pick_map[...])) + diagonal_times(x)
        wait_recv_all(giveback, rnd)
        came_back = []
        for h in range(ghost_hi):
            value = ret_buf[rnd, h * pad : (h + 1) * pad, :]
            stacked = jnp.concatenate(
                [jnp.where(send_hi[h] == i, value, 0.0) for i in range(own_hi)], axis=0
            )
            came_back.append(split3(stacked))
        result = result + sum3(dot_nt(jnp.concatenate(came_back, axis=1), send_map[...]))
        return result

    def stage1(d):
        slot = sum1.at[in_block]
        return pltpu.make_async_remote_copy(
            src_ref=slot, dst_ref=slot, send_sem=s1_send.at[d], recv_sem=s1_recv.at[d],
            device_id=(peer1(d),), device_id_type=MESH,
        )

    def stage2(d):
        slot = sum2.at[block_of]
        return pltpu.make_async_remote_copy(
            src_ref=slot, dst_ref=slot, send_sem=s2_send.at[d], recv_sem=s2_recv.at[d],
            device_id=(peer2(d),), device_id_type=MESH,
        )

    def lane_sums(x):
        total = jnp.sum(x, axis=0, keepdims=True)
        return total[:, :LANES] + total[:, LANES:]

    def pair_of(x, y):
        return jnp.concatenate([lane_sums(x), lane_sums(y)], axis=0)

    def begin_sum(x, y):
        sum1[in_block] = pair_of(x, y)
        for d in range(1, g1):
            stage1(d).start()

    def middle_sum():
        for d in range(1, g1):
            stage1(d).wait_recv()
        sum2[block_of] = jnp.sum(sum1[...], axis=0)
        for d in range(1, g2):
            stage2(d).start()

    def totals(parts):
        total = jnp.sum(jnp.sum(parts, axis=0), axis=1, keepdims=True)
        return total[0:1], total[1:2]

    def end_sum():
        for d in range(1, g2):
            stage2(d).wait_recv()
        return totals(sum2[...])

    def straight(d):
        return pltpu.make_async_remote_copy(
            src_ref=sum_all.at[0], dst_ref=sum_all.at[d],
            send_sem=all_send.at[d], recv_sem=all_recv.at[d],
            device_id=(lax.rem(me + d, n),), device_id_type=MESH,
        )

    def sum_straight(x, y):
        sum_all[0] = pair_of(x, y)
        for d in sorted(range(1, n), key=lambda d: abs(2 * d - n)):
            straight(d).start()
        for d in range(1, n):
            straight(d).wait_recv()
        return totals(sum_all[...])

    q = operate(b_buf[...], b_split, 0, lambda: None)
    q_buf[...] = q
    q_split = split3(q)
    send_of(q_split, 1)
    start_all(fetch, 1)
    b = b_buf[...]
    begin_sum(b * b, b * q)
    w = operate(q_buf[...], q_split, 1, middle_sum)
    rr, curve = end_sum()
    step0 = rr / curve
    b, q = b_buf[...], q_buf[...]
    r1 = b - step0 * q
    z1 = q - step0 * w
    new, curve = sum_straight(r1 * r1, r1 * z1)
    beta = new / rr
    step1 = new / (curve - beta * new / step0)
    sol = step0 * b + step1 * (r1 + beta * b)
    res = r1 - step1 * (z1 + beta * q)
    for h in range(own_hi):
        sol_ref[:, h * WIDE : (h + 1) * WIDE] = sol[h * pad : h * pad + trace]
        res_ref[:, h * WIDE : (h + 1) * WIDE] = res[h * pad : h * pad + trace]
    for rnd in range(2):
        wait_send_all(fetch, rnd)
        wait_send_all(giveback, rnd)
    for d in range(1, g1):
        stage1(d).wait_send()
    for d in range(1, g2):
        stage2(d).wait_send()
    for d in range(1, n):
        straight(d).wait_send()


def put_out(sol_ref, res_ref, sol_out, res_out, sems):
    copies = [
        pltpu.make_async_copy(sol_ref, sol_out, sems.at[0]),
        pltpu.make_async_copy(res_ref, res_out, sems.at[1]),
    ]
    for copy in copies:
        copy.start()
    for copy in copies:
        copy.wait()


def solution(mesh):
    n = mesh.shape["dom"]
    g1 = next(g for g in range(1, n + 1) if n % g == 0 and g * g >= n)
    g2 = n // g1

    def shards(rs, em, fm, si, sc, mass, absorb, imp):
        trace, own = rs.shape
        sides, elements = fm.shape
        blocks, width = si.shape[1:]
        pad = -(-trace // 8) * 8
        rows_own = own // WIDE * pad
        rows_ghost = blocks * width // WIDE * pad
        picks = sides * elements
        dofs = sides * trace
        cfg = (n, g1, g2, trace, sides, elements, own, blocks, width)
        dma = pltpu.SemaphoreType.DMA
        vmem = pl.BlockSpec(memory_space=pltpu.VMEM)
        sol, res = pl.pallas_call(
            functools.partial(kernel, cfg),
            out_shape=[pltpu.VMEM(rs.shape, F32)] * 2,
            in_specs=[pl.BlockSpec(memory_space=pltpu.HBM)] * 8,
            out_specs=[vmem] * 2,
            scratch_shapes=[
                pltpu.VMEM(rs.shape, F32),
                pltpu.VMEM(fm.shape, jnp.int32),
                pltpu.VMEM(si.shape, jnp.int32),
                pltpu.VMEM(sc.shape, jnp.int32),
                pltpu.VMEM((1, own), F32),
                pltpu.VMEM((1, own), jnp.int32),
                pltpu.VMEM((1, own), F32),
                pltpu.VMEM((dofs, dofs, elements), BF16),
                pltpu.VMEM((WIDE, picks), BF16),
                pltpu.VMEM((WIDE, blocks * width), BF16),
                pltpu.VMEM((2, rows_ghost, WIDE), F32),
                pltpu.VMEM((2, rows_ghost, WIDE), F32),
                pltpu.VMEM((2, rows_ghost, WIDE), F32),
                pltpu.VMEM((2, rows_ghost, WIDE), F32),
                pltpu.VMEM((sides, pad, elements), F32),
                pltpu.VMEM((dofs + 8, elements), F32),
                pltpu.VMEM((3 * rows_own, picks), BF16),
                pltpu.VMEM((3 * rows_ghost, picks), BF16),
                pltpu.VMEM((rows_own, WIDE), F32),
                pltpu.VMEM((rows_own, WIDE), F32),
                pltpu.VMEM((g1, 2, LANES), F32),
                pltpu.VMEM((g2, 2, LANES), F32),
                pltpu.VMEM((n, 2, LANES), F32),
                dma((7,)), dma((sides,)),
                dma((2, blocks)), dma((2, blocks)), dma((2, blocks)), dma((2, blocks)),
                dma((g1,)), dma((g1,)), dma((g2,)), dma((g2,)), dma((n,)), dma((n,)),
            ],
            compiler_params=pltpu.CompilerParams(
                collective_id=0, has_side_effects=True, vmem_limit_bytes=62 * 1024 * 1024
            ),
        )(rs, em, fm, si, sc, mass.reshape(1, own), absorb.reshape(1, own), imp.reshape(1, own))
        return pl.pallas_call(
            put_out,
            out_shape=[jax.ShapeDtypeStruct(rs.shape, F32)] * 2,
            in_specs=[vmem] * 2,
            out_specs=[pl.BlockSpec(memory_space=pltpu.HBM)] * 2,
            scratch_shapes=[dma((2,))],
            compiler_params=pltpu.CompilerParams(vmem_limit_bytes=8 * 1024 * 1024),
        )(sol, res)

    placed = (
        P(None, "dom"),
        P(None, None, "dom"),
        P(None, "dom"),
        P("dom", None, None),
        P("dom", None),
        P("dom"),
        P("dom"),
        P("dom"),
    )
    return jax.shard_map(
        shards,
        mesh=mesh,
        in_specs=placed,
        out_specs=(P(None, "dom"), P(None, "dom")),
        check_vma=False,
    )
```
